128 devices in a mesh: pts: 128 (over z, y, x, core).
Axes of the slice: x: 4, y: 4, z: 4, core: 2. Of those that a mesh axis runs over, the one named last changes fastest.
Arguments:
- points: bfloat16 [65536, 64], P('pts'), may hold values from -10 to 10, as said below
- targets: float32 [65536], P('pts'), may hold values from -6 to 6
- ridge_weight: float32 [], replicated, may hold values from 0.5 to 4
Outputs:
- coefficients: float32 [65536], P('pts')
- residual: float32 [65536], P('pts')
The draws below stay inside these ranges and needn't reach their ends.
Inputs may be any that keep to these rules, and one draw needn't show every extreme that they name: `points`: each point lies near one of 1365 cluster centres; every coordinate is within -10 and 10.
All inputs are finite; a program needn't handle non-finite values.
Results may differ from the reference program's by a relative error of at most 0.005.
Values may be sent and summed in bfloat16 or wider, within the bound.
A program may use at most 192 MiB of HBM per device.

```python
import math
import jax
import jax.numpy as jnp
from jax import lax

D = 64
PTS_DEV = 512
ITERS = 2
NPTS = 65536
CLUSTERS = 1365


def draw_points(key, part):
    key_centre = jax.random.fold_in(key, 11)
    key_member = jax.random.fold_in(key, 12)
    key_noise = jax.random.fold_in(key, 13)
    centres = 0.5 * jax.random.truncated_normal(key_centre, -4.0, 4.0, (CLUSTERS, D), jnp.float32)
    members = jax.random.randint(key_member, (NPTS,), 0, CLUSTERS)
    noise = 0.5 * jax.random.truncated_normal(key_noise, -4.0, 4.0, (NPTS, D), jnp.float32)
    return (centres[members] + noise).astype(jnp.bfloat16)


def level_of(rng, dims, pieces, smallest, high):
    def one(axis_at, shards_of):
        steps = jax.random.uniform(jax.random.fold_in(jax.random.fold_in(rng, 6), axis_at), (shards_of,), jnp.float32, smallest / len(pieces), high / len(pieces))
        return jnp.repeat(jnp.exp(steps), dims[axis_at] // shards_of).reshape((-1,) + (1,) * (len(dims) - axis_at - 1))

    factor_of = one(*pieces[0])
    for cut in pieces[1:]:
        factor_of = factor_of * one(*cut)
    return factor_of


def normal_values(own_key, dims, scale, bound, split=(), kind=jnp.bfloat16):
    result = scale * jax.random.normal(own_key, dims, jnp.float32)
    if split:
        result = result * level_of(own_key, dims, split, -0.22, 0.18)
    return jnp.clip(result, -bound, bound).astype(kind)


def setup_inputs(seed: int = 0) -> dict:
    arg_keys = jax.random.split(jax.random.key(seed), 4)
    points = draw_points(jax.random.fold_in(arg_keys[3], 71), 0)
    targets = normal_values(arg_keys[1], (NPTS,), 1.0, 6.0, ((0, 128),), jnp.float32)
    ridge_weight = jnp.clip(jnp.exp(jax.random.uniform(arg_keys[2], (), jnp.float32, math.log(0.5), math.log(4.0))), 0.5, 4.0)
    return dict(points=points, targets=targets, ridge_weight=ridge_weight)


def reference(points, targets, ridge_weight):
    inverse_width = 1.0 / D
    widened = points.astype(jnp.float32)
    squared = jnp.sum(widened * widened, axis=1)
    blocks = points.reshape(NPTS // PTS_DEV, PTS_DEV, D)
    block_norms = squared.reshape(NPTS // PTS_DEV, PTS_DEV)

    def apply_operator(vector):
        vector_low = vector.astype(jnp.bfloat16)

        def tile_product(operands):
            tile_rows, tile_norms = operands
            cross_term = jnp.dot(tile_rows, points.T, preferred_element_type=jnp.float32)
            distance = tile_norms[:, None] + squared[None, :] - 2.0 * cross_term
            kernel = jnp.exp(-inverse_width * distance).astype(jnp.bfloat16)
            return jnp.dot(kernel, vector_low, preferred_element_type=jnp.float32)

        summed = lax.map(tile_product, (blocks, block_norms)).reshape(NPTS)
        return summed + ridge_weight * vector

    coefficients = jnp.zeros_like(targets)
    residual = targets
    direction = targets
    norm_now = jnp.sum(residual * residual)
    for iteration in range(ITERS):
        applied = apply_operator(direction)
        step_size = norm_now / jnp.sum(direction * applied)
        coefficients = coefficients + step_size * direction
        residual = residual - step_size * applied
        norm_next = jnp.sum(residual * residual)
        direction = residual + (norm_next / norm_now) * direction
        norm_now = norm_next
    return coefficients, residual
```

```python
import math

import jax
import jax.numpy as jnp
from jax import lax
from jax.experimental import pallas as pl
from jax.experimental.pallas import tpu as pltpu
from jax.sharding import PartitionSpec as P

f32, bf16 = jnp.float32, jnp.bfloat16
BLK, DIM = 512, 64
SCALE = math.log2(math.e) / DIM
ROWS = [(dx, dc) for dx in range(4) for dc in range(2)]
COLS = [(0, 0), (0, 1), (3, 0), (1, 1), (1, 3), (3, 2), (2, 3), (0, 2), (2, 0), (2, 2)]
FULL_COLS = range(1, 7)
SELF_COLS = [0, 7, 8, 9]
FULL_ROWS = [2, 3]
SELF_ROWS = [0, 1, 4, 5]
NR, NC = len(ROWS), len(COLS)
NFULL = 8 * 6


def position():
    me = lax.axis_index("pts")
    return me // 32, (me // 8) % 4, (me // 2) % 4, me % 2


def at_rows(dx, dc):
    z, y, x, c = position()
    return ((z * 4 + y) * 4 + (x + dx) % 4) * 2 + (c + dc) % 2


def at_cols(dz, dy):
    z, y, x, c = position()
    return (((z + dz) % 4 * 4 + (y + dy) % 4) * 4 + x) * 2 + c


def send(src, dst, ssem, rsem, dev):
    cp = pltpu.make_async_remote_copy(
        src_ref=src, dst_ref=dst, send_sem=ssem, recv_sem=rsem,
        device_id=(dev,), device_id_type=pl.DeviceIdType.MESH)
    cp.start()
    return cp


def low(v):
    return v.astype(bf16).astype(f32)


def three(v):
    hi = low(v)
    mid = low(v - hi)
    return hi, mid, low(v - hi - mid)


def put_rows(parts, first):
    row = lax.broadcasted_iota(jnp.int32, (16, BLK), 0)
    tile = jnp.where((row >= 3 - first) & (row < 6 - first), 1.0, 0.0).astype(f32)
    for k, part in enumerate(parts):
        tile = jnp.where(row == first + k, jnp.broadcast_to(part, (16, BLK)), tile)
    return tile.astype(bf16)


def build_left(raw, left):
    wide = raw.astype(f32)
    norm = -SCALE * jnp.sum(wide * wide, axis=0, keepdims=True)
    rows = put_rows(three(norm), 0)
    stack = jnp.concatenate([raw, raw, raw, rows, jnp.zeros((48, BLK), bf16)], axis=0)
    left[...] = stack.T


def build_right(raw, right):
    wide = raw.astype(f32)
    norm = -SCALE * jnp.sum(wide * wide, axis=0, keepdims=True)
    hi, mid, lo = three(wide * (2.0 * SCALE))
    right[0:64, :] = hi.astype(bf16)
    right[64:128, :] = mid.astype(bf16)
    right[128:192, :] = lo.astype(bf16)
    right[192:208, :] = put_rows(three(norm), 3)
    right[208:256, :] = jnp.zeros((48, BLK), bf16)


def half(k):
    return pl.ds(pl.multiple_of(k * 256, 256), 256)


def which_half(r, c):
    z, y, x, core = position()
    dz, dy = COLS[c]
    dx, dc = ROWS[r]
    if dz:
        return z // 2
    if dy:
        return y // 2
    if dx:
        return x // 2
    return core


def entries(left, right):
    return jnp.exp2(jnp.dot(left, right, preferred_element_type=f32)).astype(bf16)


def across(kernel, vec, first):
    wide = kernel.astype(f32)
    out = None
    for q in range(wide.shape[1] // 128):
        term = wide[:, 128 * q:128 * (q + 1)] * vec[pl.ds(first + q, 1), :]
        out = term if out is None else out + term
    return out


def fill_vectors(tile, rows_vec, cols_vec, exact):
    hi = low(tile)
    lo = low(tile - hi) if exact else jnp.zeros_like(tile)
    if cols_vec is not None:
        cols_vec[...] = tile if exact else hi
    if rows_vec is not None:
        for q in range(4):
            both = jnp.concatenate([jnp.broadcast_to(hi[q:q + 1, :], (8, 128)),
                                    jnp.broadcast_to(lo[q:q + 1, :], (8, 128))], axis=0)
            rows_vec[:, 128 * q:128 * (q + 1)] = both.astype(bf16)


def kernel(pts_ref, tgt_ref, ridge_ref, coef_ref, res_ref,
           raw_r, raw_c, left, right, kst, kdiag, t_r, t_c, y_r, y_c, vr, vc, prow, pcol,
           out_r, out_c, in1_r, in1_c, in2_r, in2_c, sc_out, sc1, sc2,
           s_raw, q_raw_r, q_raw_c, s_t, q_t_r, q_t_c, s_part, q_part, s_y, q_y_r, q_y_c,
           s_sc, q_sc):
    ridge = ridge_ref[0]
    raw_r[0] = pts_ref[...].astype(f32).T.astype(bf16)
    own_t = jnp.concatenate([tgt_ref[...], jnp.zeros((4, 128), f32)], axis=0)
    t_r[0] = own_t

    barrier = pltpu.get_barrier_semaphore()
    for r in range(1, NR):
        pl.semaphore_signal(barrier, inc=1, device_id=(at_rows(*ROWS[r]),), device_id_type=pl.DeviceIdType.MESH)
    for k in range(1, 16):
        pl.semaphore_signal(barrier, inc=1, device_id=(at_cols(k // 4, k % 4),), device_id_type=pl.DeviceIdType.MESH)
    build_left(raw_r[0], left.at[0])
    build_right(raw_r[0], right.at[0])
    pl.semaphore_wait(barrier, NR - 1 + 15)

    raws = {}
    for r in (1, 2, 6, 4):
        dx, dc = ROWS[r]
        raws[r] = send(raw_r.at[0], raw_r.at[r], s_raw.at[r], q_raw_r.at[r], at_rows(-dx, -dc))
    for c in range(1, NC):
        dz, dy = COLS[c]
        raws[NR + c] = send(raw_r.at[0], raw_c.at[c], s_raw.at[NR + c], q_raw_c.at[c], at_cols(-dz, -dy))
    ts = []
    for r in range(1, NR):
        dx, dc = ROWS[r]
        ts.append(send(t_r.at[0], t_r.at[r], s_t.at[r], q_t_r.at[r], at_rows(-dx, -dc)))
    for c in range(1, NC):
        dz, dy = COLS[c]
        ts.append(send(t_r.at[0], t_c.at[c], s_t.at[NR + c], q_t_c.at[c], at_cols(-dz, -dy)))

    for r in (2, 6, 4):
        raws[r].wait_recv()
        raws[r + 1] = send(raw_r.at[r], raw_r.at[r + 1], s_raw.at[r + 1], q_raw_r.at[r + 1], at_rows(0, 1))
        build_left(raw_r[r], left.at[r])
    for r in (1, 3, 7, 5):
        raws[r].wait_recv()
        build_left(raw_r[r], left.at[r])

    def form_full(t, r, c):
        for h in range(2):
            kst[t, 256 * h:256 * (h + 1), :] = entries(left[r, 256 * h:256 * (h + 1), :], right[c])

    def form_self(x):
        c = SELF_COLS[x]
        for i, r in enumerate(FULL_ROWS):
            form_full(NFULL + 4 * x + i, r, c)
        for j, r in enumerate(SELF_ROWS):
            t, rows = NFULL + 4 * x + 2 + j // 2, pl.ds(256 * (j % 2), 256)
            if x == 0 and j == 0:
                kdiag[...] = entries(left[0, 256:512, :], right[0, :, 256:512])
                kst[t, rows, :] = entries(left[0, 0:256, :], right[0])
            else:
                b = which_half(r, c)
                kst[t, rows, 0:256] = entries(left[r, half(b), :], right[c, :, half(b)])
                kst[t, rows, 256:512] = entries(left[r, 0:256, :], right[c, :, 256:512])

    form_self(0)

    def form_cols(c, carry):
        pltpu.make_async_copy(raw_c.at[c], raw_c.at[c], q_raw_c.at[c]).wait()
        build_right(raw_c[c], right.at[c])
        for r in range(NR):
            form_full((c - 1) * NR + r, r, c)
        return carry

    lax.fori_loop(1, 7, form_cols, 0)
    for x in (1, 2, 3):
        c = SELF_COLS[x]
        raws[NR + c].wait_recv()
        build_right(raw_c[c], right.at[c])
        form_self(x)
    for cp in raws.values():
        cp.wait_send()

    def multiply():
        for r in range(NR):
            prow[r] = jnp.zeros((BLK, 128), f32)
        for c in range(NC):
            pcol[c] = jnp.zeros((16, BLK), f32)

        def tile(t, r, c):
            for k in range(8):
                rows = pl.ds(64 * k, 64)
                prow[r, rows, :] += across(kst[t, rows, :], vc.at[c], 0)
            return jnp.dot(vr[r], kst[t], preferred_element_type=f32)

        def cols(c, carry):
            total = None
            for r in range(NR):
                part = tile((c - 1) * NR + r, r, c)
                total = part if total is None else total + part
            pcol[c] = total
            return carry

        def quad(k_ref, r, c, p, q, both):
            for k in range(4):
                rows = pl.ds(pl.multiple_of(p * 256 + 64 * k, 64), 64)
                prow[r, rows, :] += across(k_ref[64 * k:64 * (k + 1), :], vc.at[c], 2 * q)
            if both:
                pcol[c, :, half(q)] += jnp.dot(vr[r, :, half(p)], k_ref[...], preferred_element_type=f32)

        def selfs(x):
            c = SELF_COLS[x]
            total = None
            for i, r in enumerate(FULL_ROWS):
                part = tile(NFULL + 4 * x + i, r, c)
                total = part if total is None else total + part
            pcol[c] = total
            for j, r in enumerate(SELF_ROWS):
                t, rows = NFULL + 4 * x + 2 + j // 2, pl.ds(256 * (j % 2), 256)
                diag = x == 0 and j == 0
                b = 0 if diag else which_half(r, c)
                quad(kst.at[t, rows, 0:256], r, c, b, b, not diag)
                quad(kst.at[t, rows, 256:512], r, c, 0, 1, True)
            if x == 0:
                quad(kdiag, 0, 0, 1, 1, False)

        lax.fori_loop(1, 7, cols, 0)
        for x in range(4):
            selfs(x)

    def row_share(r):
        rows = [jnp.sum(prow[r, 128 * q:128 * (q + 1), :].T, axis=0, keepdims=True) for q in range(4)]
        return jnp.concatenate(rows + [jnp.zeros((4, 128), f32)], axis=0)

    def col_share(c):
        both = pcol[c, 0:1, :] + pcol[c, 8:9, :]
        rows = [both[:, 128 * q:128 * (q + 1)] for q in range(4)]
        return jnp.concatenate(rows + [jnp.zeros((4, 128), f32)], axis=0)

    def exchange(in_r, in_c):
        cps = []
        for c in range(1, NC):
            out_c[c] = col_share(c)
            cps.append(send(out_c.at[c], in_c.at[c], s_part.at[NR + c], q_part.at[NR + c], at_cols(*COLS[c])))
        for r in range(1, NR):
            out_r[r] = row_share(r)
            cps.append(send(out_r.at[r], in_r.at[r], s_part.at[r], q_part.at[r], at_rows(*ROWS[r])))
        out_r[0] = row_share(0)
        out_c[0] = col_share(0)
        return cps

    def gathered(cps, in_r, in_c):
        total = out_r[0] + out_c[0]
        for cp in cps:
            cp.wait_recv()
        for c in range(1, NC):
            total += in_c[c]
        for r in range(1, NR):
            total += in_r[r]
        for cp in cps:
            cp.wait_send()
        return total

    for r in range(1, NR):
        ts[r - 1].wait_recv()
    for c in range(1, NC):
        ts[NR - 2 + c].wait_recv()
    for r in range(NR):
        fill_vectors(t_r[r], vr.at[r], vc.at[0] if r == 0 else None, False)
    for c in range(1, NC):
        fill_vectors(t_c[c], None, vc.at[c], False)
    multiply()
    cps = exchange(in1_r, in1_c)
    for cp in ts:
        cp.wait_send()
    t_own = t_r[0]
    y_own = gathered(cps, in1_r, in1_c) + ridge * t_own
    y_r[0] = y_own

    ys = []
    for c in range(1, NC):
        dz, dy = COLS[c]
        ys.append(send(y_r.at[0], y_c.at[c], s_y.at[NR + c], q_y_c.at[c], at_cols(-dz, -dy)))
    for r in range(1, NR):
        dx, dc = ROWS[r]
        ys.append(send(y_r.at[0], y_r.at[r], s_y.at[r], q_y_r.at[r], at_rows(-dx, -dc)))

    lane_row = lax.broadcasted_iota(jnp.int32, (8, 128), 0)

    def spread(values):
        out = jnp.zeros((8, 128), f32)
        for k, value in enumerate(values):
            whole = jnp.sum(jnp.sum(value, axis=0, keepdims=True), axis=1, keepdims=True)
            out = jnp.where(lane_row == k, jnp.broadcast_to(whole, (8, 128)), out)
        return out

    def stage_one(n):
        cps = []
        for r in range(1, NR):
            dx, dc = ROWS[r]
            cps.append(send(sc_out.at[n], sc1.at[n, r], s_sc.at[n, r], q_sc.at[n, r], at_rows(-dx, -dc)))
        return cps

    def stage_two(n, cps):
        total = sc_out[n]
        for r, cp in enumerate(cps):
            cp.wait_recv()
            total += sc1[n, r + 1]
        sc_out[2 + n] = total
        more = []
        for k in range(1, 16):
            more.append(send(sc_out.at[2 + n], sc2.at[n, k], s_sc.at[n, NR + k], q_sc.at[n, NR + k],
                             at_cols(-(k // 4), -(k % 4))))
        return more

    def stage_three(n, cps, more):
        total = sc_out[2 + n]
        for k, cp in enumerate(more):
            cp.wait_recv()
            total += sc2[n, k + 1]
        for cp in cps + more:
            cp.wait_send()
        return total

    sc_out[0] = spread([t_own * t_own, t_own * y_own, y_own * y_own])
    first = stage_one(0)

    for cp in ys:
        cp.wait_recv()
    for r in range(NR):
        fill_vectors(y_r[r], vr.at[r], vc.at[0] if r == 0 else None, True)
    for c in range(1, NC):
        fill_vectors(y_c[c], None, vc.at[c], True)
    second = stage_two(0, first)
    multiply()
    cps = exchange(in2_r, in2_c)
    dot = y_own * (out_r[0] + out_c[0] + ridge * y_own)
    for r in range(1, NR):
        dot += y_r[r] * out_r[r]
    for c in range(1, NC):
        dot += y_c[c] * out_c[c]
    sc_out[1] = spread([dot])
    third = stage_one(1)
    sums = stage_three(0, first, second)
    fourth = stage_two(1, third)
    for cp in ys:
        cp.wait_send()
    w_own = gathered(cps, in2_r, in2_c) + ridge * y_own
    tt, ty, yy = sums[0:1, :], sums[1:2, :], sums[2:3, :]
    alpha = tt / ty
    next_norm = alpha * alpha * yy - tt
    beta = next_norm / tt
    yw = stage_three(1, third, fourth)[0:1, :]
    curve = (1.0 + beta) * ((1.0 + beta) * ty - 2.0 * alpha * yy) + alpha * alpha * yw
    alpha2 = next_norm / curve
    res1 = t_own - alpha * y_own
    dir2 = res1 + beta * t_own
    app2 = (1.0 + beta) * y_own - alpha * w_own
    coef_ref[...] = (alpha * t_own + alpha2 * dir2)[0:4, :]
    res_ref[...] = (res1 - alpha2 * app2)[0:4, :]


def body(points, targets, ridge_weight):
    vmem = pl.BlockSpec(memory_space=pltpu.VMEM)
    dma = pltpu.SemaphoreType.DMA
    out = jax.ShapeDtypeStruct((4, 128), f32)
    coef, res = pl.pallas_call(
        kernel,
        out_shape=(out, out),
        in_specs=[vmem, vmem, pl.BlockSpec(memory_space=pltpu.SMEM)],
        out_specs=(vmem, vmem),
        scratch_shapes=[
            pltpu.VMEM((NR, DIM, BLK), bf16), pltpu.VMEM((NC, DIM, BLK), bf16),
            pltpu.VMEM((NR, BLK, 256), bf16), pltpu.VMEM((NC, 256, BLK), bf16),
            pltpu.VMEM((NFULL + 16, BLK, BLK), bf16), pltpu.VMEM((256, 256), bf16),
            pltpu.VMEM((NR, 8, 128), f32), pltpu.VMEM((NC, 8, 128), f32),
            pltpu.VMEM((NR, 8, 128), f32), pltpu.VMEM((NC, 8, 128), f32),
            pltpu.VMEM((NR, 16, BLK), bf16), pltpu.VMEM((NC, 8, 128), f32),
            pltpu.VMEM((NR, BLK, 128), f32), pltpu.VMEM((NC, 16, BLK), f32),
            pltpu.VMEM((NR, 8, 128), f32), pltpu.VMEM((NC, 8, 128), f32),
            pltpu.VMEM((NR, 8, 128), f32), pltpu.VMEM((NC, 8, 128), f32),
            pltpu.VMEM((NR, 8, 128), f32), pltpu.VMEM((NC, 8, 128), f32),
            pltpu.VMEM((4, 8, 128), f32), pltpu.VMEM((2, NR, 8, 128), f32), pltpu.VMEM((2, 16, 8, 128), f32),
            dma((NR + NC,)), dma((NR,)), dma((NC,)),
            dma((NR + NC,)), dma((NR,)), dma((NC,)),
            dma((NR + NC,)), dma((NR + NC,)),
            dma((NR + NC,)), dma((NR,)), dma((NC,)),
            dma((2, NR + 16)), dma((2, NR + 16)),
        ],
        compiler_params=pltpu.CompilerParams(
            collective_id=0, has_side_effects=True, vmem_limit_bytes=60 * 2 ** 20),
        name="cg",
    )(points, targets.reshape(4, 128), ridge_weight.reshape(1))
    return coef.reshape(-1), res.reshape(-1)


def solution(mesh):
    in_specs = (P("pts", None), P("pts"), P())
    out_specs = (P("pts"), P("pts"))
    return jax.shard_map(body, mesh=mesh, in_specs=in_specs, out_specs=out_specs, check_vma=False)
```

```python
import math

import jax
import jax.numpy as jnp
from jax import lax
from jax.experimental import pallas as pl
from jax.experimental.pallas import tpu as pltpu
from jax.sharding import PartitionSpec as P

f32, bf16 = jnp.float32, jnp.bfloat16
BLK, DIM = 512, 64
SCALE = math.log2(math.e) / DIM
ROWS = [(dx, dc) for dx in range(4) for dc in range(2)]
COLS = [(0, 0), (0, 1), (3, 0), (1, 1), (1, 3), (3, 2), (2, 3), (0, 2), (2, 0), (2, 2)]
FULL_COLS = range(1, 7)
SELF_COLS = [0, 7, 8, 9]
FULL_ROWS = [2, 3]
SELF_ROWS = [0, 1, 4, 5]
NR, NC = len(ROWS), len(COLS)
NFULL = 8 * 6


def position():
    me = lax.axis_index("pts")
    return me // 32, (me // 8) % 4, (me // 2) % 4, me % 2


def at_rows(dx, dc):
    z, y, x, c = position()
    return ((z * 4 + y) * 4 + (x + dx) % 4) * 2 + (c + dc) % 2


def at_cols(dz, dy):
    z, y, x, c = position()
    return (((z + dz) % 4 * 4 + (y + dy) % 4) * 4 + x) * 2 + c


def send(src, dst, ssem, rsem, dev):
    cp = pltpu.make_async_remote_copy(
        src_ref=src, dst_ref=dst, send_sem=ssem, recv_sem=rsem,
        device_id=(dev,), device_id_type=pl.DeviceIdType.MESH)
    cp.start()
    return cp


def low(v):
    return v.astype(bf16).astype(f32)


def three(v):
    hi = low(v)
    mid = low(v - hi)
    return hi, mid, low(v - hi - mid)


def put_rows(parts, first):
    row = lax.broadcasted_iota(jnp.int32, (16, BLK), 0)
    tile = jnp.where((row >= 3 - first) & (row < 6 - first), 1.0, 0.0).astype(f32)
    for k, part in enumerate(parts):
        tile = jnp.where(row == first + k, jnp.broadcast_to(part, (16, BLK)), tile)
    return tile.astype(bf16)


def build_left(raw, left):
    wide = raw.astype(f32)
    norm = -SCALE * jnp.sum(wide * wide, axis=0, keepdims=True)
    rows = put_rows(three(norm), 0)
    stack = jnp.concatenate([raw, raw, raw, rows, jnp.zeros((48, BLK), bf16)], axis=0)
    left[...] = stack.T


def build_right(raw, right):
    wide = raw.astype(f32)
    norm = -SCALE * jnp.sum(wide * wide, axis=0, keepdims=True)
    hi, mid, lo = three(wide * (2.0 * SCALE))
    right[0:64, :] = hi.astype(bf16)
    right[64:128, :] = mid.astype(bf16)
    right[128:192, :] = lo.astype(bf16)
    right[192:208, :] = put_rows(three(norm), 3)
    right[208:256, :] = jnp.zeros((48, BLK), bf16)


def half(k):
    return pl.ds(pl.multiple_of(k * 256, 256), 256)


def which_half(r, c):
    z, y, x, core = position()
    dz, dy = COLS[c]
    dx, dc = ROWS[r]
    if dz:
        return z // 2
    if dy:
        return y // 2
    if dx:
        return x // 2
    return core


def entries(left, right):
    return jnp.exp2(jnp.dot(left, right, preferred_element_type=f32)).astype(bf16)


def across(kernel, vec, first):
    wide = kernel.astype(f32)
    out = None
    for q in range(wide.shape[1] // 128):
        term = wide[:, 128 * q:128 * (q + 1)] * vec[pl.ds(first + q, 1), :]
        out = term if out is None else out + term
    return out


def fill_vectors(tile, rows_vec, cols_vec, exact):
    hi = low(tile)
    lo = low(tile - hi) if exact else jnp.zeros_like(tile)
    if cols_vec is not None:
        cols_vec[...] = tile if exact else hi
    if rows_vec is not None:
        for q in range(4):
            both = jnp.concatenate([jnp.broadcast_to(hi[q:q + 1, :], (8, 128)),
                                    jnp.broadcast_to(lo[q:q + 1, :], (8, 128))], axis=0)
            rows_vec[:, 128 * q:128 * (q + 1)] = both.astype(bf16)


def kernel(pts_ref, tgt_ref, ridge_ref, coef_ref, res_ref,
           raw_r, raw_c, left, right, kst, kdiag, t_r, t_c, y_r, y_c, vr, vc, prow, pcol,
           out_r, out_c, in1_r, in1_c, in2_r, in2_c, sc_out, sc1, sc2,
           s_raw, q_raw_r, q_raw_c, s_t, q_t_r, q_t_c, s_part, q_part, s_y, q_y_r, q_y_c,
           s_sc, q_sc):
    ridge = ridge_ref[0]
    raw_r[0] = pts_ref[...]
    own_t = jnp.concatenate([tgt_ref[...], jnp.zeros((4, 128), f32)], axis=0)
    t_r[0] = own_t

    barrier = pltpu.get_barrier_semaphore()
    for r in range(1, NR):
        pl.semaphore_signal(barrier, inc=1, device_id=(at_rows(*ROWS[r]),), device_id_type=pl.DeviceIdType.MESH)
    for k in range(1, 16):
        pl.semaphore_signal(barrier, inc=1, device_id=(at_cols(k // 4, k % 4),), device_id_type=pl.DeviceIdType.MESH)
    build_left(raw_r[0], left.at[0])
    build_right(raw_r[0], right.at[0])
    kdiag[...] = entries(left[0, 256:512, :], right[0, :, 256:512])
    kst[NFULL + 2, 0:256, :] = entries(left[0, 0:256, :], right[0])
    prow[...] = jnp.zeros((NR, BLK, 128), f32)
    pl.semaphore_wait(barrier, NR - 1 + 15)

    raws = {}
    for r in (1, 2, 6):
        dx, dc = ROWS[r]
        raws[r] = send(raw_r.at[0], raw_r.at[r], s_raw.at[r], q_raw_r.at[r], at_rows(-dx, -dc))

    def send_col(c):
        dz, dy = COLS[c]
        raws[NR + c] = send(raw_r.at[0], raw_c.at[c], s_raw.at[NR + c], q_raw_c.at[c], at_cols(-dz, -dy))

    for c in (1, 2):
        send_col(c)
    raws[4] = send(raw_r.at[0], raw_r.at[4], s_raw.at[4], q_raw_r.at[4], at_rows(-2, 0))
    for c in range(3, NC):
        send_col(c)
    ts = []
    for r in range(1, NR):
        dx, dc = ROWS[r]
        ts.append(send(t_r.at[0], t_r.at[r], s_t.at[r], q_t_r.at[r], at_rows(-dx, -dc)))
    for c in range(1, NC):
        dz, dy = COLS[c]
        ts.append(send(t_r.at[0], t_c.at[c], s_t.at[NR + c], q_t_c.at[c], at_cols(-dz, -dy)))

    def take_row(r):
        raws[r].wait_recv()
        if r in (2, 6, 4):
            raws[r + 1] = send(raw_r.at[r], raw_r.at[r + 1], s_raw.at[r + 1], q_raw_r.at[r + 1], at_rows(0, 1))
        build_left(raw_r[r], left.at[r])

    def take_col(c):
        pltpu.make_async_copy(raw_c.at[c], raw_c.at[c], q_raw_c.at[c]).wait()
        build_right(raw_c[c], right.at[c])

    def form_full(t, r, c):
        for h in range(2):
            kst[t, 256 * h:256 * (h + 1), :] = entries(left[r, 256 * h:256 * (h + 1), :], right[c])

    def form_cols(c, rows):
        for r in rows:
            form_full((c - 1) * NR + r, r, c)

    def form_self(x):
        c = SELF_COLS[x]
        for i, r in enumerate(FULL_ROWS):
            form_full(NFULL + 4 * x + i, r, c)
        for j, r in enumerate(SELF_ROWS):
            if x == 0 and j == 0:
                continue
            t, rows = NFULL + 4 * x + 2 + j // 2, pl.ds(256 * (j % 2), 256)
            b = which_half(r, c)
            kst[t, rows, 0:256] = entries(left[r, half(b), :], right[c, :, half(b)])
            kst[t, rows, 256:512] = entries(left[r, 0:256, :], right[c, :, 256:512])

    near, far = (0, 1, 2, 6), (3, 7, 4, 5)
    for r in near[1:]:
        take_row(r)

    def form_near(c, carry):
        take_col(c)
        form_cols(c, near)
        return carry

    def form_far(c, carry):
        form_cols(c, far)
        return carry

    lax.fori_loop(1, 4, form_near, 0)
    take_row(4)
    take_row(3)
    take_row(7)
    lax.fori_loop(4, 5, form_near, 0)
    take_row(5)
    lax.fori_loop(1, 5, form_far, 0)
    form_self(0)
    for c in (5, 6):
        take_col(c)
        form_cols(c, range(NR))
    for x in (1, 2, 3):
        take_col(SELF_COLS[x])
        form_self(x)
    for cp in raws.values():
        cp.wait_send()

    def row_share(r):
        rows = [jnp.sum(prow[r, 128 * q:128 * (q + 1), :].T, axis=0, keepdims=True) for q in range(4)]
        return jnp.concatenate(rows + [jnp.zeros((4, 128), f32)], axis=0)

    def col_share(c):
        both = pcol[c, 0:1, :] + pcol[c, 8:9, :]
        rows = [both[:, 128 * q:128 * (q + 1)] for q in range(4)]
        return jnp.concatenate(rows + [jnp.zeros((4, 128), f32)], axis=0)

    def ship(in_c, n, c, dz, dy):
        out_c[c] = col_share(c)
        send(out_c.at[c], in_c.at[c], s_part.at[NR + c], q_part.at[n, NR + c], at_cols(dz, dy))

    def multiply(in_r, in_c, n):
        def along(t, r, c):
            for k in range(8):
                rows = pl.ds(64 * k, 64)
                prow[r, rows, :] += across(kst[t, rows, :], vc.at[c], 0)

        def along_quad(k_ref, r, c, p, q):
            for k in range(4):
                rows = pl.ds(pl.multiple_of(p * 256 + 64 * k, 64), 64)
                prow[r, rows, :] += across(k_ref[64 * k:64 * (k + 1), :], vc.at[c], 2 * q)

        def along_self(x):
            c = SELF_COLS[x]
            for i, r in enumerate(FULL_ROWS):
                along(NFULL + 4 * x + i, r, c)
            for j, r in enumerate(SELF_ROWS):
                t, rows = NFULL + 4 * x + 2 + j // 2, pl.ds(256 * (j % 2), 256)
                b = 0 if x == 0 and j == 0 else which_half(r, c)
                along_quad(kst.at[t, rows, 0:256], r, c, b, b)
                along_quad(kst.at[t, rows, 256:512], r, c, 0, 1)
            if x == 0:
                along_quad(kdiag, 0, 0, 1, 1)

        def down_full(base, rows, c):
            total = None
            for i, r in enumerate(rows):
                part = jnp.dot(vr[r], kst[base + i], preferred_element_type=f32)
                total = part if total is None else total + part
            pcol[c] = total

        def down(c):
            down_full((c - 1) * NR, range(NR), c)

        def down_self(x):
            c = SELF_COLS[x]
            down_full(NFULL + 4 * x, FULL_ROWS, c)
            for j, r in enumerate(SELF_ROWS):
                t, rows = NFULL + 4 * x + 2 + j // 2, pl.ds(256 * (j % 2), 256)
                if not (x == 0 and j == 0):
                    b = which_half(r, c)
                    pcol[c, :, half(b)] += jnp.dot(vr[r, :, half(b)], kst[t, rows, 0:256], preferred_element_type=f32)
                pcol[c, :, 256:512] += jnp.dot(vr[r, :, 0:256], kst[t, rows, 256:512], preferred_element_type=f32)

        def vector(c):
            if n:
                pltpu.make_async_copy(y_c.at[c], y_c.at[c], q_y_c.at[c]).wait()
                fill_vectors(y_c[c], None, vc.at[c], True)

        for x in (3, 2, 1):
            down_self(x)
        along_self(0)
        for x in (3, 2, 1):
            ship(in_c, n, SELF_COLS[x], *COLS[SELF_COLS[x]])

        def step(i, code):
            vector(i)
            down(7 - i)
            for r in range(NR):
                along((i - 1) * NR + r, r, i)
            ship(in_c, n, 7 - i, code // 4 % 4, code % 4)
            return code // 16

        codes = sum((4 * COLS[7 - i][0] + COLS[7 - i][1]) * 16 ** (i - 1) for i in range(1, 6))
        lax.fori_loop(1, 6, step, jnp.int32(codes))
        for x in (1, 2, 3):
            vector(SELF_COLS[x])
        vector(6)
        down(1)
        down_self(0)
        for x in (1, 2, 3):
            along_self(x)
        ship(in_c, n, 1, *COLS[1])
        for r in (4, 5, 2, 3, 6, 7, 1, 0):
            along(5 * NR + r, r, 6)
            out_r[r] = row_share(r)
        cps = []
        for r in (4, 5, 2, 3, 6, 7, 1):
            cps.append(send(out_r.at[r], in_r.at[r], s_part.at[r], q_part.at[n, r], at_rows(*ROWS[r])))
        out_c[0] = col_share(0)
        return cps

    def gathered(cps, in_r, in_c, n):
        total = out_r[0] + out_c[0]
        for c in range(1, NC):
            pltpu.make_async_copy(in_c.at[c], in_c.at[c], q_part.at[n, NR + c]).wait()
            total += in_c[c]
        for cp in cps:
            cp.wait_recv()
        for r in range(1, NR):
            total += in_r[r]
        for cp in cps:
            cp.wait_send()
        for c in range(1, NC):
            pltpu.make_async_copy(out_c.at[c], out_c.at[c], s_part.at[NR + c]).wait()
        return total

    for cp in ts:
        cp.wait_recv()
    for r in range(NR):
        fill_vectors(t_r[r], vr.at[r], vc.at[0] if r == 0 else None, False)
    for c in range(1, NC):
        fill_vectors(t_c[c], None, vc.at[c], False)
    cps = multiply(in1_r, in1_c, 0)
    for cp in ts:
        cp.wait_send()
    t_own = t_r[0]
    y_own = gathered(cps, in1_r, in1_c, 0) + ridge * t_own
    y_r[0] = y_own

    ys = []
    for r in range(1, NR):
        dx, dc = ROWS[r]
        ys.append(send(y_r.at[0], y_r.at[r], s_y.at[r], q_y_r.at[r], at_rows(-dx, -dc)))
    for c in range(1, NC):
        dz, dy = COLS[c]
        ys.append(send(y_r.at[0], y_c.at[c], s_y.at[NR + c], q_y_c.at[c], at_cols(-dz, -dy)))

    lane_row = lax.broadcasted_iota(jnp.int32, (8, 128), 0)

    def spread(values):
        out = jnp.zeros((8, 128), f32)
        for k, value in enumerate(values):
            whole = jnp.sum(jnp.sum(value, axis=0, keepdims=True), axis=1, keepdims=True)
            out = jnp.where(lane_row == k, jnp.broadcast_to(whole, (8, 128)), out)
        return out

    def stage_one(n):
        cps = []
        for r in range(1, NR):
            dx, dc = ROWS[r]
            cps.append(send(sc_out.at[n], sc1.at[n, r], s_sc.at[n, r], q_sc.at[n, r], at_rows(-dx, -dc)))
        return cps

    def stage_two(n, cps):
        total = sc_out[n]
        for r, cp in enumerate(cps):
            cp.wait_recv()
            total += sc1[n, r + 1]
        sc_out[2 + n] = total
        more = []
        for k in range(1, 16):
            more.append(send(sc_out.at[2 + n], sc2.at[n, k], s_sc.at[n, NR + k], q_sc.at[n, NR + k],
                             at_cols(-(k // 4), -(k % 4))))
        return more

    def stage_three(n, cps, more):
        total = sc_out[2 + n]
        for k, cp in enumerate(more):
            cp.wait_recv()
            total += sc2[n, k + 1]
        for cp in cps + more:
            cp.wait_send()
        return total

    sc_out[0] = spread([t_own * t_own, t_own * y_own, y_own * y_own])
    first = stage_one(0)
    prow[...] = jnp.zeros((NR, BLK, 128), f32)

    fill_vectors(y_own, vr.at[0], vc.at[0], True)
    for r in range(1, NR):
        ys[r - 1].wait_recv()
        fill_vectors(y_r[r], vr.at[r], None, True)
    second = stage_two(0, first)
    cps = multiply(in2_r, in2_c, 1)
    dot = y_own * (out_r[0] + out_c[0] + ridge * y_own)
    for r in range(1, NR):
        dot += y_r[r] * out_r[r]
    for c in range(1, NC):
        dot += y_c[c] * out_c[c]
    sc_out[1] = spread([dot])
    third = stage_one(1)
    sums = stage_three(0, first, second)
    fourth = stage_two(1, third)
    for cp in ys:
        cp.wait_send()
    w_own = gathered(cps, in2_r, in2_c, 1) + ridge * y_own
    tt, ty, yy = sums[0:1, :], sums[1:2, :], sums[2:3, :]
    alpha = tt / ty
    next_norm = alpha * alpha * yy - tt
    beta = next_norm / tt
    yw = stage_three(1, third, fourth)[0:1, :]
    curve = (1.0 + beta) * ((1.0 + beta) * ty - 2.0 * alpha * yy) + alpha * alpha * yw
    alpha2 = next_norm / curve
    res1 = t_own - alpha * y_own
    dir2 = res1 + beta * t_own
    app2 = (1.0 + beta) * y_own - alpha * w_own
    coef_ref[...] = (alpha * t_own + alpha2 * dir2)[0:4, :]
    res_ref[...] = (res1 - alpha2 * app2)[0:4, :]


def body(points, targets, ridge_weight):
    vmem = pl.BlockSpec(memory_space=pltpu.VMEM)
    dma = pltpu.SemaphoreType.DMA
    out = jax.ShapeDtypeStruct((4, 128), f32)
    coef, res = pl.pallas_call(
        kernel,
        out_shape=(out, out),
        in_specs=[vmem, vmem, pl.BlockSpec(memory_space=pltpu.SMEM)],
        out_specs=(vmem, vmem),
        scratch_shapes=[
            pltpu.VMEM((NR, DIM, BLK), bf16), pltpu.VMEM((NC, DIM, BLK), bf16),
            pltpu.VMEM((NR, BLK, 256), bf16), pltpu.VMEM((NC, 256, BLK), bf16),
            pltpu.VMEM((NFULL + 16, BLK, BLK), bf16), pltpu.VMEM((256, 256), bf16),
            pltpu.VMEM((NR, 8, 128), f32), pltpu.VMEM((NC, 8, 128), f32),
            pltpu.VMEM((NR, 8, 128), f32), pltpu.VMEM((NC, 8, 128), f32),
            pltpu.VMEM((NR, 16, BLK), bf16), pltpu.VMEM((NC, 8, 128), f32),
            pltpu.VMEM((NR, BLK, 128), f32), pltpu.VMEM((NC, 16, BLK), f32),
            pltpu.VMEM((NR, 8, 128), f32), pltpu.VMEM((NC, 8, 128), f32),
            pltpu.VMEM((NR, 8, 128), f32), pltpu.VMEM((NC, 8, 128), f32),
            pltpu.VMEM((NR, 8, 128), f32), pltpu.VMEM((NC, 8, 128), f32),
            pltpu.VMEM((4, 8, 128), f32), pltpu.VMEM((2, NR, 8, 128), f32), pltpu.VMEM((2, 16, 8, 128), f32),
            dma((NR + NC,)), dma((NR,)), dma((NC,)),
            dma((NR + NC,)), dma((NR,)), dma((NC,)),
            dma((NR + NC,)), dma((2, NR + NC)),
            dma((NR + NC,)), dma((NR,)), dma((NC,)),
            dma((2, NR + 16)), dma((2, NR + 16)),
        ],
        compiler_params=pltpu.CompilerParams(
            collective_id=0, has_side_effects=True, vmem_limit_bytes=60 * 2 ** 20),
        name="cg",
    )(points.T, targets.reshape(4, 128), ridge_weight.reshape(1))
    return coef.reshape(-1), res.reshape(-1)


def solution(mesh):
    in_specs = (P("pts", None), P("pts"), P())
    out_specs = (P("pts"), P("pts"))
    return jax.shard_map(body, mesh=mesh, in_specs=in_specs, out_specs=out_specs, check_vma=False)
```

```python
import math

import jax
import jax.numpy as jnp
from jax import lax
from jax.experimental import pallas as pl
from jax.experimental.pallas import tpu as pltpu
from jax.sharding import PartitionSpec as P

f32, bf16 = jnp.float32, jnp.bfloat16
BLK, DIM = 512, 64
SCALE = math.log2(math.e) / DIM
ROWS = [(dx, dc) for dx in range(4) for dc in range(2)]
COLS = [(0, 0), (0, 1), (3, 0), (1, 1), (1, 3), (3, 2), (2, 3), (0, 2), (2, 0), (2, 2)]
FULL_COLS = range(1, 7)
SELF_COLS = [0, 7, 8, 9]
FULL_ROWS = [2, 3]
SELF_ROWS = [0, 1, 4, 5]
NR, NC = len(ROWS), len(COLS)
NFULL = 8 * 6


def position():
    me = lax.axis_index("pts")
    return me // 32, (me // 8) % 4, (me // 2) % 4, me % 2


def at_rows(dx, dc):
    z, y, x, c = position()
    return ((z * 4 + y) * 4 + (x + dx) % 4) * 2 + (c + dc) % 2


def at_cols(dz, dy):
    z, y, x, c = position()
    return (((z + dz) % 4 * 4 + (y + dy) % 4) * 4 + x) * 2 + c


def send(src, dst, ssem, rsem, dev):
    cp = pltpu.make_async_remote_copy(
        src_ref=src, dst_ref=dst, send_sem=ssem, recv_sem=rsem,
        device_id=(dev,), device_id_type=pl.DeviceIdType.MESH)
    cp.start()
    return cp


def low(v):
    return v.astype(bf16).astype(f32)


def three(v):
    hi = low(v)
    mid = low(v - hi)
    return hi, mid, low(v - hi - mid)


def put_rows(parts, first):
    row = lax.broadcasted_iota(jnp.int32, (16, BLK), 0)
    tile = jnp.where((row >= 3 - first) & (row < 6 - first), 1.0, 0.0).astype(f32)
    for k, part in enumerate(parts):
        tile = jnp.where(row == first + k, jnp.broadcast_to(part, (16, BLK)), tile)
    return tile.astype(bf16)


def build_left(raw, left):
    wide = raw.astype(f32)
    norm = -SCALE * jnp.sum(wide * wide, axis=0, keepdims=True)
    rows = put_rows(three(norm), 0)
    stack = jnp.concatenate([raw, raw, raw, rows, jnp.zeros((48, BLK), bf16)], axis=0)
    left[...] = stack.T


def build_right(raw, right):
    wide = raw.astype(f32)
    norm = -SCALE * jnp.sum(wide * wide, axis=0, keepdims=True)
    hi, mid, lo = three(wide * (2.0 * SCALE))
    right[0:64, :] = hi.astype(bf16)
    right[64:128, :] = mid.astype(bf16)
    right[128:192, :] = lo.astype(bf16)
    right[192:208, :] = put_rows(three(norm), 3)
    right[208:256, :] = jnp.zeros((48, BLK), bf16)


def half(k):
    return pl.ds(pl.multiple_of(k * 256, 256), 256)


def which_half(r, c):
    z, y, x, core = position()
    dz, dy = COLS[c]
    dx, dc = ROWS[r]
    if dz:
        return z // 2
    if dy:
        return y // 2
    if dx:
        return x // 2
    return core


def entries(left, right):
    return jnp.exp2(jnp.dot(left, right, preferred_element_type=f32)).astype(bf16)


def across(kernel, vec, first):
    wide = kernel.astype(f32)
    out = None
    for q in range(wide.shape[1] // 128):
        term = wide[:, 128 * q:128 * (q + 1)] * vec[pl.ds(first + q, 1), :]
        out = term if out is None else out + term
    return out


def fill_vectors(tile, rows_vec, cols_vec, exact):
    hi = low(tile)
    lo = low(tile - hi) if exact else jnp.zeros_like(tile)
    if cols_vec is not None:
        cols_vec[...] = tile if exact else hi
    if rows_vec is not None:
        for q in range(4):
            both = jnp.concatenate([jnp.broadcast_to(hi[q:q + 1, :], (8, 128)),
                                    jnp.broadcast_to(lo[q:q + 1, :], (8, 128))], axis=0)
            rows_vec[:, 128 * q:128 * (q + 1)] = both.astype(bf16)


def kernel(pts_ref, tgt_ref, ridge_ref, coef_ref, res_ref,
           raw_r, raw_c, left, right, kst, kdiag, t_r, t_c, y_r, y_c, vr, vc, prow, pcol,
           out_r, out_c, in_r, in_c, sc_out, sc_in,
           s_raw, q_raw_r, q_raw_c, s_t, q_t_r, q_t_c, s_part, q_part, s_y, q_y_r, q_y_c,
           s_sc, q_sc, rounds):
    ridge = ridge_ref[0]
    raw_r[0] = pts_ref[...]
    t_r[0] = jnp.concatenate([tgt_ref[...], jnp.zeros((4, 128), f32)], axis=0)

    def greet(sem):
        for dev in (at_rows(0, 1), at_rows(1, 0), at_rows(3, 0), at_cols(0, 1), at_cols(0, 3), at_cols(1, 0), at_cols(3, 0)):
            pl.semaphore_signal(sem, inc=1, device_id=(dev,), device_id_type=pl.DeviceIdType.MESH)

    barrier = pltpu.get_barrier_semaphore()
    greet(barrier)
    build_left(raw_r[0], left.at[0])
    build_right(raw_r[0], right.at[0])
    kdiag[...] = entries(left[0, 256:512, :], right[0, :, 256:512])
    kst[NFULL + 2, 0:256, :] = entries(left[0, 0:256, :], right[0])
    pl.semaphore_wait(barrier, 7)

    raws = {}

    def send_row(r):
        dx, dc = ROWS[r]
        raws[r] = send(raw_r.at[0], raw_r.at[r], s_raw.at[r], q_raw_r.at[r], at_rows(-dx, -dc))

    def send_col(c):
        dz, dy = COLS[c]
        raws[NR + c] = send(raw_r.at[0], raw_c.at[c], s_raw.at[NR + c], q_raw_c.at[c], at_cols(-dz, -dy))

    def take_row(r):
        raws[r].wait_recv()
        if r in (2, 6, 4):
            raws[r + 1] = send(raw_r.at[r], raw_r.at[r + 1], s_raw.at[r + 1], q_raw_r.at[r + 1], at_rows(0, 1))
        build_left(raw_r[r], left.at[r])

    def take_col(c):
        raws[NR + c].wait_recv()
        build_right(raw_c[c], right.at[c])

    def form_full(t, r, c):
        for h in range(2):
            kst[t, 256 * h:256 * (h + 1), :] = entries(left[r, 256 * h:256 * (h + 1), :], right[c])

    def form(cols, rows):
        for c in cols:
            for r in rows:
                form_full((c - 1) * NR + r, r, c)

    def form_self(x):
        c = SELF_COLS[x]
        for i, r in enumerate(FULL_ROWS):
            form_full(NFULL + 4 * x + i, r, c)
        for j, r in enumerate(SELF_ROWS):
            if x == 0 and j == 0:
                continue
            t, rows = NFULL + 4 * x + 2 + j // 2, pl.ds(256 * (j % 2), 256)
            b = which_half(r, c)
            kst[t, rows, 0:256] = entries(left[r, half(b), :], right[c, :, half(b)])
            kst[t, rows, 256:512] = entries(left[r, 0:256, :], right[c, :, 256:512])

    for r in (1, 2, 6):
        send_row(r)
    send_col(1)
    send_col(2)
    greet(rounds.at[0])
    prow[...] = jnp.zeros((NR, BLK, 128), f32)
    pl.semaphore_wait(rounds.at[0], 7)
    greet(rounds.at[1])
    send_row(4)
    send_col(3)
    send_col(4)
    take_row(1)
    pl.semaphore_wait(rounds.at[1], 7)
    greet(rounds.at[2])
    take_row(2)
    take_row(6)
    for c in (5, 6, 7, 8):
        send_col(c)
    take_col(1)
    form((1,), (0, 1, 2, 6))
    pl.semaphore_wait(rounds.at[2], 7)
    send_col(9)
    ts = {}
    for r in range(1, NR):
        dx, dc = ROWS[r]
        ts[r] = send(t_r.at[0], t_r.at[r], s_t.at[r], q_t_r.at[r], at_rows(-dx, -dc))
    for c in range(1, NC):
        dz, dy = COLS[c]
        ts[NR + c] = send(t_r.at[0], t_c.at[c], s_t.at[NR + c], q_t_c.at[c], at_cols(-dz, -dy))
    take_col(2)
    take_row(3)
    take_row(7)
    form((2,), (0, 1, 2, 6, 3, 7))
    form((1,), (3, 7))
    take_row(4)
    take_col(3)
    form((3,), (0, 1, 2, 6, 3, 7))
    take_row(5)
    take_col(4)
    form((4,), range(NR))
    form((1, 2, 3), (4, 5))
    form_self(0)
    for c in (5, 6):
        take_col(c)
        form((c,), range(NR))
    for x in (1, 2, 3):
        take_col(SELF_COLS[x])
        form_self(x)
    for cp in raws.values():
        cp.wait_send()

    def row_share(r):
        rows = [jnp.sum(prow[r, 128 * q:128 * (q + 1), :].T, axis=0, keepdims=True) for q in range(4)]
        return jnp.concatenate(rows + [jnp.zeros((4, 128), f32)], axis=0)

    def col_share(c):
        both = pcol[c, 0:1, :] + pcol[c, 8:9, :]
        rows = [both[:, 128 * q:128 * (q + 1)] for q in range(4)]
        return jnp.concatenate(rows + [jnp.zeros((4, 128), f32)], axis=0)

    def along_rows(t, r, c):
        for k in range(8):
            rows = pl.ds(64 * k, 64)
            prow[r, rows, :] += across(kst[t, rows, :], vc.at[c], 0)

    def along_quad(k_ref, r, c, p, q):
        for k in range(4):
            rows = pl.ds(pl.multiple_of(p * 256 + 64 * k, 64), 64)
            prow[r, rows, :] += across(k_ref[64 * k:64 * (k + 1), :], vc.at[c], 2 * q)

    def pair(r, c):
        if c in FULL_COLS:
            return (c - 1) * NR + r, None
        x = SELF_COLS.index(c)
        if r in FULL_ROWS:
            return NFULL + 4 * x + FULL_ROWS.index(r), None
        if r in SELF_ROWS:
            j = SELF_ROWS.index(r)
            return NFULL + 4 * x + 2 + j // 2, pl.ds(256 * (j % 2), 256)
        return None, None

    def along(r, c):
        t, rows = pair(r, c)
        if rows is None:
            along_rows(t, r, c)
            return
        b = 0 if r == 0 and c == 0 else which_half(r, c)
        along_quad(kst.at[t, rows, 0:256], r, c, b, b)
        along_quad(kst.at[t, rows, 256:512], r, c, 0, 1)
        if r == 0 and c == 0:
            along_quad(kdiag, 0, 0, 1, 1)

    def down(r, c, first):
        t, rows = pair(r, c)
        if rows is None:
            part = jnp.dot(vr[r], kst[t], preferred_element_type=f32)
            pcol[c] = part if first else pcol[c] + part
            return
        if not (r == 0 and c == 0):
            b = which_half(r, c)
            pcol[c, :, half(b)] += jnp.dot(vr[r, :, half(b)], kst[t, rows, 0:256], preferred_element_type=f32)
        pcol[c, :, 256:512] += jnp.dot(vr[r, :, 0:256], kst[t, rows, 256:512], preferred_element_type=f32)

    def along_list(rows, cols):
        return [(r, c) for c in cols for r in rows if pair(r, c)[0] is not None]

    def down_list(cols):
        out = []
        for c in cols:
            rows = range(NR) if c in FULL_COLS else FULL_ROWS + SELF_ROWS
            out += [(r, c, i == 0) for i, r in enumerate(rows)]
        return out

    def weave(alongs, downs):
        done = 0
        for i, item in enumerate(alongs):
            along(*item)
            upto = (i + 1) * len(downs) // len(alongs)
            for extra in downs[done:upto]:
                down(*extra)
            done = upto

    def multiply(n):
        cps = []

        def vectors(cols):
            for c in cols if n else ():
                ys[NR + c].wait_recv()
                fill_vectors(y_c[c], None, vc.at[c], True)

        def ship_cols(cols):
            for c in cols:
                out_c[c] = col_share(c)
            for c in cols:
                cps.append(send(out_c.at[c], in_c.at[n, c], s_part.at[n, NR + c], q_part.at[n, NR + c], at_cols(*COLS[c])))

        def ship_rows(rows):
            for r in rows:
                out_r[r] = row_share(r)
            for r in rows:
                cps.append(send(out_r.at[r], in_r.at[n, r], s_part.at[n, r], q_part.at[n, r], at_rows(*ROWS[r])))

        rows_a, rows_b, rows_c = (4, 5), (2, 3, 6, 7), (0, 1)
        if n:
            weave(along_list(range(NR), (0,)), [])
            vectors((1, 2))
            weave(along_list(range(NR), (1, 2)), [])
            for r in range(1, NR):
                ys[r].wait_recv()
                fill_vectors(y_r[r], vr.at[r], None, True)
            vectors((3, 4))
            weave(along_list(rows_a, (3, 4)), down_list((9,)))
            vectors((5, 6, 7, 8, 9))
            weave(along_list(rows_a, (5, 6, 7, 8, 9)), down_list((8, 7, 6)))
            ship_cols((9, 8, 7, 6))
            ship_rows(rows_a)
            weave(along_list(rows_b, range(3, NC)), down_list((5, 4, 3, 2, 1)))
            ship_cols((5, 4, 3, 2, 1))
            ship_rows(rows_b)
            weave(along_list(rows_c, range(3, NC)), down_list((0,)))
        else:
            weave(along_list(rows_a, range(NC)), down_list((9, 8, 7, 6)))
            ship_cols((9, 8, 7, 6))
            ship_rows(rows_a)
            weave(along_list(rows_b, range(NC)), down_list((5, 4, 3, 2, 1)))
            ship_cols((5, 4, 3, 2, 1))
            ship_rows(rows_b)
            weave(along_list(rows_c, range(NC)), down_list((0,)))
        out_r[1] = row_share(1)
        cps.append(send(out_r.at[1], in_r.at[n, 1], s_part.at[n, 1], q_part.at[n, 1], at_rows(*ROWS[1])))
        out_r[0] = row_share(0)
        out_c[0] = col_share(0)
        return cps

    def gathered(cps, n):
        total = out_r[0] + out_c[0]
        for cp in cps:
            cp.wait_recv()
        for c in range(1, NC):
            total += in_c[n, c]
        for r in range(1, NR):
            total += in_r[n, r]
        for cp in cps:
            cp.wait_send()
        return total

    for cp in ts.values():
        cp.wait_recv()
    for r in range(NR):
        fill_vectors(t_r[r], vr.at[r], vc.at[0] if r == 0 else None, False)
    for c in range(1, NC):
        fill_vectors(t_c[c], None, vc.at[c], False)
    cps = multiply(0)
    for cp in ts.values():
        cp.wait_send()
    t_own = t_r[0]
    y_own = gathered(cps, 0) + ridge * t_own
    y_r[0] = y_own

    ys = {}
    for r in range(1, NR):
        dx, dc = ROWS[r]
        ys[r] = send(y_r.at[0], y_r.at[r], s_y.at[r], q_y_r.at[r], at_rows(-dx, -dc))
    for c in range(1, NC):
        dz, dy = COLS[c]
        ys[NR + c] = send(y_r.at[0], y_c.at[c], s_y.at[NR + c], q_y_c.at[c], at_cols(-dz, -dy))

    lane = lax.broadcasted_iota(jnp.int32, (1, 128), 1)
    me = lax.axis_index("pts")

    def total_send(n, values):
        out = jnp.zeros((1, 128), f32)
        for k, value in enumerate(values):
            whole = jnp.sum(jnp.sum(value, axis=0, keepdims=True), axis=1, keepdims=True)
            out = jnp.where(lane == k, jnp.broadcast_to(whole, (1, 128)), out)
        sc_out[n] = out

        def one(k, carry):
            send(sc_out.at[n], sc_in.at[n, k], s_sc.at[n], q_sc.at[n], (me + k) % 128)
            return carry

        lax.fori_loop(1, 128, one, 0)

    def total_wait(n):
        every = sc_in.at[n, pl.ds(1, 127)]
        pltpu.make_async_copy(every, every, q_sc.at[n]).wait()
        out = sc_out[n] + jnp.sum(sc_in[n, 1:128], axis=0)
        pltpu.make_async_copy(every, every, s_sc.at[n]).wait()
        return out

    total_send(0, [t_own * t_own, t_own * y_own, y_own * y_own])
    prow[...] = jnp.zeros((NR, BLK, 128), f32)

    fill_vectors(y_own, vr.at[0], vc.at[0], True)
    cps = multiply(1)
    dot = y_own * (out_r[0] + out_c[0] + ridge * y_own)
    for r in range(1, NR):
        dot += y_r[r] * out_r[r]
    for c in range(1, NC):
        dot += y_c[c] * out_c[c]
    total_send(1, [dot])
    sums = total_wait(0)
    for cp in ys.values():
        cp.wait_send()
    w_own = gathered(cps, 1) + ridge * y_own
    tt, ty, yy = sums[:, 0:1], sums[:, 1:2], sums[:, 2:3]
    alpha = tt / ty
    next_norm = alpha * alpha * yy - tt
    beta = next_norm / tt
    res1 = t_own - alpha * y_own
    dir2 = res1 + beta * t_own
    app2 = (1.0 + beta) * y_own - alpha * w_own
    part = (1.0 + beta) * ((1.0 + beta) * ty - 2.0 * alpha * yy)
    alpha2 = next_norm / (part + alpha * alpha * total_wait(1)[:, 0:1])
    coef_ref[...] = (alpha * t_own + alpha2 * dir2)[0:4, :]
    res_ref[...] = (res1 - alpha2 * app2)[0:4, :]


def body(points, targets, ridge_weight):
    vmem = pl.BlockSpec(memory_space=pltpu.VMEM)
    dma = pltpu.SemaphoreType.DMA
    out = jax.ShapeDtypeStruct((4, 128), f32)
    coef, res = pl.pallas_call(
        kernel,
        out_shape=(out, out),
        in_specs=[vmem, vmem, pl.BlockSpec(memory_space=pltpu.SMEM)],
        out_specs=(vmem, vmem),
        scratch_shapes=[
            pltpu.VMEM((NR, DIM, BLK), bf16), pltpu.VMEM((NC, DIM, BLK), bf16),
            pltpu.VMEM((NR, BLK, 256), bf16), pltpu.VMEM((NC, 256, BLK), bf16),
            pltpu.VMEM((NFULL + 16, BLK, BLK), bf16), pltpu.VMEM((256, 256), bf16),
            pltpu.VMEM((NR, 8, 128), f32), pltpu.VMEM((NC, 8, 128), f32),
            pltpu.VMEM((NR, 8, 128), f32), pltpu.VMEM((NC, 8, 128), f32),
            pltpu.VMEM((NR, 16, BLK), bf16), pltpu.VMEM((NC, 8, 128), f32),
            pltpu.VMEM((NR, BLK, 128), f32), pltpu.VMEM((NC, 16, BLK), f32),
            pltpu.VMEM((NR, 8, 128), f32), pltpu.VMEM((NC, 8, 128), f32),
            pltpu.VMEM((2, NR, 8, 128), f32), pltpu.VMEM((2, NC, 8, 128), f32),
            pltpu.VMEM((2, 1, 128), f32), pltpu.VMEM((2, 128, 1, 128), f32),
            dma((NR + NC,)), dma((NR,)), dma((NC,)),
            dma((NR + NC,)), dma((NR,)), dma((NC,)),
            dma((2, NR + NC)), dma((2, NR + NC)),
            dma((NR + NC,)), dma((NR,)), dma((NC,)),
            dma((2,)), dma((2,)), pltpu.SemaphoreType.REGULAR((3,)),
        ],
        compiler_params=pltpu.CompilerParams(
            collective_id=0, has_side_effects=True, vmem_limit_bytes=60 * 2 ** 20),
        name="cg",
    )(points.T, targets.reshape(4, 128), ridge_weight.reshape(1))
    return coef.reshape(-1), res.reshape(-1)


def solution(mesh):
    in_specs = (P("pts", None), P("pts"), P())
    out_specs = (P("pts"), P("pts"))
    return jax.shard_map(body, mesh=mesh, in_specs=in_specs, out_specs=out_specs, check_vma=False)
```

```python
import math

import jax
import jax.numpy as jnp
from jax import lax
from jax.experimental import pallas as pl
from jax.experimental.pallas import tpu as pltpu
from jax.sharding import PartitionSpec as P

f32, bf16 = jnp.float32, jnp.bfloat16
BLK, DIM = 512, 64
SCALE = math.log2(math.e) / DIM
ROWS = [(dx, dc) for dx in range(4) for dc in range(2)]
COLS = [(0, 0), (0, 1), (1, 0), (1, 1), (3, 1), (3, 2), (2, 3), (0, 2), (2, 0), (2, 2)]
FULL_COLS = range(1, 7)
SELF_COLS = [0, 7, 8, 9]
FULL_ROWS = [2, 3]
SELF_ROWS = [0, 1, 4, 5]
NR, NC = len(ROWS), len(COLS)
NFULL = 8 * 6


def position():
    me = lax.axis_index("pts")
    return me // 32, (me // 8) % 4, (me // 2) % 4, me % 2


def at_rows(dx, dc):
    z, y, x, c = position()
    return ((z * 4 + y) * 4 + (x + dx) % 4) * 2 + (c + dc) % 2


def at_cols(dz, dy):
    z, y, x, c = position()
    return (((z + dz) % 4 * 4 + (y + dy) % 4) * 4 + x) * 2 + c


def send(src, dst, ssem, rsem, dev):
    cp = pltpu.make_async_remote_copy(
        src_ref=src, dst_ref=dst, send_sem=ssem, recv_sem=rsem,
        device_id=(dev,), device_id_type=pl.DeviceIdType.MESH)
    cp.start()
    return cp


def low(v):
    return v.astype(bf16).astype(f32)


def three(v):
    hi = low(v)
    mid = low(v - hi)
    return hi, mid, low(v - hi - mid)


def put_rows(parts, first):
    row = lax.broadcasted_iota(jnp.int32, (16, BLK), 0)
    tile = jnp.where((row >= 3 - first) & (row < 6 - first), 1.0, 0.0).astype(f32)
    for k, part in enumerate(parts):
        tile = jnp.where(row == first + k, jnp.broadcast_to(part, (16, BLK)), tile)
    return tile.astype(bf16)


def build_left(raw, left):
    wide = raw.astype(f32)
    norm = -SCALE * jnp.sum(wide * wide, axis=0, keepdims=True)
    rows = put_rows(three(norm), 0)
    stack = jnp.concatenate([raw, raw, raw, rows, jnp.zeros((48, BLK), bf16)], axis=0)
    left[...] = stack.T


def build_right(raw, right):
    wide = raw.astype(f32)
    norm = -SCALE * jnp.sum(wide * wide, axis=0, keepdims=True)
    hi, mid, lo = three(wide * (2.0 * SCALE))
    right[0:64, :] = hi.astype(bf16)
    right[64:128, :] = mid.astype(bf16)
    right[128:192, :] = lo.astype(bf16)
    right[192:208, :] = put_rows(three(norm), 3)
    right[208:256, :] = jnp.zeros((48, BLK), bf16)


def half(k):
    return pl.ds(pl.multiple_of(k * 256, 256), 256)


def which_half(r, c):
    z, y, x, core = position()
    dz, dy = COLS[c]
    dx, dc = ROWS[r]
    if dz:
        return z // 2
    if dy:
        return y // 2
    if dx:
        return x // 2
    return core


def entries(left, right):
    return jnp.exp2(jnp.dot(left, right, preferred_element_type=f32)).astype(bf16)


def across(kernel, vec, first):
    wide = kernel.astype(f32)
    out = None
    for q in range(wide.shape[1] // 128):
        term = wide[:, 128 * q:128 * (q + 1)] * vec[pl.ds(first + q, 1), :]
        out = term if out is None else out + term
    return out


def fill_vectors(tile, rows_vec, cols_vec, exact):
    hi = low(tile)
    lo = low(tile - hi) if exact else jnp.zeros_like(tile)
    if cols_vec is not None:
        cols_vec[...] = tile if exact else hi
    if rows_vec is not None:
        for q in range(4):
            both = jnp.concatenate([jnp.broadcast_to(hi[q:q + 1, :], (8, 128)),
                                    jnp.broadcast_to(lo[q:q + 1, :], (8, 128))], axis=0)
            rows_vec[:, 128 * q:128 * (q + 1)] = both.astype(bf16)


def kernel(pts_ref, tgt_ref, ridge_ref, coef_ref, res_ref,
           raw_r, raw_c, left, right, kst, kdiag, t_r, t_c, y_r, y_c, vr, vc, prow, pcol,
           out_r, out_c, in_r, in_c, sc_out, sc_in,
           s_raw, q_raw_r, q_raw_c, s_t, q_t_r, q_t_c, s_part, q_part, s_y, q_y_r, q_y_c,
           s_sc, q_sc, rounds):
    ridge = ridge_ref[0]
    raw_r[0] = pts_ref[...]
    t_r[0] = jnp.concatenate([tgt_ref[...], jnp.zeros((4, 128), f32)], axis=0)

    def greet(sem):
        for dev in (at_rows(0, 1), at_rows(1, 0), at_rows(3, 0), at_cols(0, 1), at_cols(0, 3), at_cols(1, 0), at_cols(3, 0)):
            pl.semaphore_signal(sem, inc=1, device_id=(dev,), device_id_type=pl.DeviceIdType.MESH)

    barrier = pltpu.get_barrier_semaphore()
    greet(barrier)
    build_left(raw_r[0], left.at[0])
    build_right(raw_r[0], right.at[0])
    kdiag[...] = entries(left[0, 256:512, :], right[0, :, 256:512])
    kst[NFULL + 2, 0:256, :] = entries(left[0, 0:256, :], right[0])
    pl.semaphore_wait(barrier, 7)

    raws = {}

    def pass_row(r, src, dx, dc):
        raws[r] = send(raw_r.at[src], raw_r.at[r], s_raw.at[r], q_raw_r.at[r], at_rows(dx, dc))

    def pass_col(c, src, dz, dy):
        raws[NR + c] = send(src, raw_c.at[c], s_raw.at[NR + c], q_raw_c.at[c], at_cols(dz, dy))

    def take_row(r):
        raws[r].wait_recv()
        if r in (2, 6, 4):
            pass_row(r + 1, r, 0, 1)
        build_left(raw_r[r], left.at[r])

    def take_col(c):
        raws[NR + c].wait_recv()
        if c == 1:
            pass_col(3, raw_c.at[1], 3, 0)
            pass_col(4, raw_c.at[1], 1, 0)
            pass_col(7, raw_c.at[1], 0, 3)
        if c == 2:
            pass_col(8, raw_c.at[2], 3, 0)
        if c == 7:
            pass_col(5, raw_c.at[7], 1, 0)
        if c == 8:
            pass_col(6, raw_c.at[8], 0, 1)
        if c == 6:
            pass_col(9, raw_c.at[6], 0, 1)
        build_right(raw_c[c], right.at[c])

    def fence():
        pl.delay(1)

    def form_full(t, r, c):
        for h in range(2):
            kst[t, 256 * h:256 * (h + 1), :] = entries(left[r, 256 * h:256 * (h + 1), :], right[c])

    def form(cols, rows):
        for c in cols:
            for r in rows:
                form_full((c - 1) * NR + r, r, c)

    def form_self(x):
        c = SELF_COLS[x]
        for i, r in enumerate(FULL_ROWS):
            form_full(NFULL + 4 * x + i, r, c)
        for j, r in enumerate(SELF_ROWS):
            if x == 0 and j == 0:
                continue
            t, rows = NFULL + 4 * x + 2 + j // 2, pl.ds(256 * (j % 2), 256)
            b = which_half(r, c)
            kst[t, rows, 0:256] = entries(left[r, half(b), :], right[c, :, half(b)])
            kst[t, rows, 256:512] = entries(left[r, 0:256, :], right[c, :, 256:512])

    core = lax.axis_index("pts") % 2
    pass_row(2, 0, 3, 0)
    pass_row(6, 0, 1, 0)
    pass_col(1, raw_r.at[0], 0, 3)
    pass_col(2, raw_r.at[0], 3, 0)
    pass_row(1, 0, 0, 1)
    greet(rounds.at[0])
    prow[...] = jnp.zeros((NR, BLK, 128), f32)
    take_row(1)
    take_row(2)
    take_row(6)
    pass_row(4, 2 + 4 * core, 3 + 2 * core, 0)
    take_col(1)
    take_col(2)
    fence()
    form((1,), (0, 1, 2, 6))
    fence()
    pl.semaphore_wait(rounds.at[0], 7)
    greet(rounds.at[1])
    take_row(3)
    take_row(7)
    fence()
    form((2,), (0, 1, 2, 6, 3, 7))
    form((1,), (3, 7))
    fence()
    take_row(4)
    take_col(7)
    take_col(8)
    take_col(3)
    take_col(4)
    fence()
    form((3,), (0, 1, 2, 6, 3, 7))
    fence()
    pl.semaphore_wait(rounds.at[1], 7)
    greet(rounds.at[2])
    take_row(5)
    fence()
    form((4,), range(NR))
    fence()
    take_col(6)
    take_col(5)
    fence()
    form((1, 2, 3), (4, 5))
    form_self(0)
    fence()
    pl.semaphore_wait(rounds.at[2], 7)
    ts = {}
    for r in range(1, NR):
        dx, dc = ROWS[r]
        ts[r] = send(t_r.at[0], t_r.at[r], s_t.at[r], q_t_r.at[r], at_rows(-dx, -dc))
    for c in range(1, NC):
        dz, dy = COLS[c]
        ts[NR + c] = send(t_r.at[0], t_c.at[c], s_t.at[NR + c], q_t_c.at[c], at_cols(-dz, -dy))
    fence()
    form_self(1)
    form_self(2)
    fence()
    form((5,), range(NR))
    fence()
    form((6,), range(NR))
    fence()
    take_col(9)
    form_self(3)
    fence()
    for cp in raws.values():
        cp.wait_send()

    def row_share(r):
        rows = [jnp.sum(prow[r, 128 * q:128 * (q + 1), :].T, axis=0, keepdims=True) for q in range(4)]
        return jnp.concatenate(rows + [jnp.zeros((4, 128), f32)], axis=0)

    def col_share(c):
        both = pcol[c, 0:1, :] + pcol[c, 8:9, :]
        rows = [both[:, 128 * q:128 * (q + 1)] for q in range(4)]
        return jnp.concatenate(rows + [jnp.zeros((4, 128), f32)], axis=0)

    def along_rows(t, r, c):
        for k in range(8):
            rows = pl.ds(64 * k, 64)
            prow[r, rows, :] += across(kst[t, rows, :], vc.at[c], 0)

    def along_quad(k_ref, r, c, p, q):
        for k in range(4):
            rows = pl.ds(pl.multiple_of(p * 256 + 64 * k, 64), 64)
            prow[r, rows, :] += across(k_ref[64 * k:64 * (k + 1), :], vc.at[c], 2 * q)

    def pair(r, c):
        if c in FULL_COLS:
            return (c - 1) * NR + r, None
        x = SELF_COLS.index(c)
        if r in FULL_ROWS:
            return NFULL + 4 * x + FULL_ROWS.index(r), None
        if r in SELF_ROWS:
            j = SELF_ROWS.index(r)
            return NFULL + 4 * x + 2 + j // 2, pl.ds(256 * (j % 2), 256)
        return None, None

    def along(r, c):
        t, rows = pair(r, c)
        if rows is None:
            along_rows(t, r, c)
            return
        b = 0 if r == 0 and c == 0 else which_half(r, c)
        along_quad(kst.at[t, rows, 0:256], r, c, b, b)
        along_quad(kst.at[t, rows, 256:512], r, c, 0, 1)
        if r == 0 and c == 0:
            along_quad(kdiag, 0, 0, 1, 1)

    def down(r, c, first):
        t, rows = pair(r, c)
        if rows is None:
            part = jnp.dot(vr[r], kst[t], preferred_element_type=f32)
            pcol[c] = part if first else pcol[c] + part
            return
        if not (r == 0 and c == 0):
            b = which_half(r, c)
            pcol[c, :, half(b)] += jnp.dot(vr[r, :, half(b)], kst[t, rows, 0:256], preferred_element_type=f32)
        pcol[c, :, 256:512] += jnp.dot(vr[r, :, 0:256], kst[t, rows, 256:512], preferred_element_type=f32)

    def along_list(rows, cols):
        return [(r, c) for c in cols for r in rows if pair(r, c)[0] is not None]

    def down_list(cols):
        out = []
        for c in cols:
            rows = range(NR) if c in FULL_COLS else FULL_ROWS + SELF_ROWS
            out += [(r, c, i == 0) for i, r in enumerate(rows)]
        return out

    def weave(alongs, downs):
        done = 0
        for i, item in enumerate(alongs):
            along(*item)
            upto = (i + 1) * len(downs) // len(alongs)
            for extra in downs[done:upto]:
                down(*extra)
            done = upto

    def multiply(n):
        cps = []

        def vectors(cols):
            for c in cols if n else ():
                ys[NR + c].wait_recv()
                fill_vectors(y_c[c], None, vc.at[c], True)

        def ship_cols(cols):
            for c in cols:
                out_c[c] = col_share(c)
            for c in cols:
                cps.append(send(out_c.at[c], in_c.at[n, c], s_part.at[n, NR + c], q_part.at[n, NR + c], at_cols(*COLS[c])))

        def ship_rows(rows):
            for r in rows:
                out_r[r] = row_share(r)
            for r in rows:
                cps.append(send(out_r.at[r], in_r.at[n, r], s_part.at[n, r], q_part.at[n, r], at_rows(*ROWS[r])))

        rows_a, rows_b, rows_c = (4, 5), (2, 3, 6, 7), (0, 1)
        if n:
            fence()
            weave(along_list(range(NR), (0,)), [])
            fence()
            vectors((1, 2))
            fence()
            weave(along_list(range(NR), (1, 2)), [])
            fence()
            for r in range(1, NR):
                ys[r].wait_recv()
                fill_vectors(y_r[r], vr.at[r], None, True)
            vectors((3, 4))
            fence()
            weave(along_list(rows_a, (3, 4)), down_list((9,)))
            fence()
            vectors((5, 6, 7, 8, 9))
            fence()
            weave(along_list(rows_a, (5, 6, 7, 8, 9)), down_list((5, 6, 7)))
            fence()
            ship_cols((9, 5, 6, 7))
            ship_rows(rows_a)
            fence()
            weave(along_list(rows_b, range(3, NC)), down_list((8, 3, 4, 2, 1)))
            fence()
            ship_cols((8, 3, 4, 2, 1))
            ship_rows(rows_b)
            fence()
            weave(along_list(rows_c, range(3, NC)), down_list((0,)))
            fence()
        else:
            fence()
            weave(along_list(rows_a, range(NC)), down_list((9, 5, 6, 7)))
            fence()
            ship_cols((9, 5, 6, 7))
            ship_rows(rows_a)
            fence()
            weave(along_list(rows_b, range(NC)), down_list((8, 3, 4, 2, 1)))
            fence()
            ship_cols((8, 3, 4, 2, 1))
            ship_rows(rows_b)
            fence()
            weave(along_list(rows_c, range(NC)), down_list((0,)))
            fence()
        out_r[1] = row_share(1)
        cps.append(send(out_r.at[1], in_r.at[n, 1], s_part.at[n, 1], q_part.at[n, 1], at_rows(*ROWS[1])))
        out_r[0] = row_share(0)
        out_c[0] = col_share(0)
        return cps

    def gathered(cps, n):
        total = out_r[0] + out_c[0]
        for cp in cps:
            cp.wait_recv()
        for c in range(1, NC):
            total += in_c[n, c]
        for r in range(1, NR):
            total += in_r[n, r]
        for cp in cps:
            cp.wait_send()
        return total

    for cp in ts.values():
        cp.wait_recv()
    for r in range(NR):
        fill_vectors(t_r[r], vr.at[r], vc.at[0] if r == 0 else None, False)
    for c in range(1, NC):
        fill_vectors(t_c[c], None, vc.at[c], False)
    cps = multiply(0)
    for cp in ts.values():
        cp.wait_send()
    t_own = t_r[0]
    y_own = gathered(cps, 0) + ridge * t_own
    y_r[0] = y_own

    ys = {}
    for r in range(1, NR):
        dx, dc = ROWS[r]
        ys[r] = send(y_r.at[0], y_r.at[r], s_y.at[r], q_y_r.at[r], at_rows(-dx, -dc))
    for c in range(1, NC):
        dz, dy = COLS[c]
        ys[NR + c] = send(y_r.at[0], y_c.at[c], s_y.at[NR + c], q_y_c.at[c], at_cols(-dz, -dy))

    lane = lax.broadcasted_iota(jnp.int32, (1, 128), 1)
    me = lax.axis_index("pts")

    def total_send(n, values):
        out = jnp.zeros((1, 128), f32)
        for k, value in enumerate(values):
            whole = jnp.sum(jnp.sum(value, axis=0, keepdims=True), axis=1, keepdims=True)
            out = jnp.where(lane == k, jnp.broadcast_to(whole, (1, 128)), out)
        sc_out[n] = out

        def one(k, carry):
            send(sc_out.at[n], sc_in.at[n, k], s_sc.at[n], q_sc.at[n], (me + k) % 128)
            return carry

        def some(i, carry):
            for j in range(16):
                one(16 * i + j + 1, carry)
            return carry

        lax.fori_loop(0, 7, some, 0)
        for k in range(113, 128):
            one(k, 0)

    def total_wait(n):
        every = sc_in.at[n, pl.ds(1, 127)]
        pltpu.make_async_copy(every, every, q_sc.at[n]).wait()
        out = sc_out[n] + jnp.sum(sc_in[n, 1:128], axis=0)
        pltpu.make_async_copy(every, every, s_sc.at[n]).wait()
        return out

    total_send(0, [t_own * t_own, t_own * y_own, y_own * y_own])
    prow[...] = jnp.zeros((NR, BLK, 128), f32)

    fill_vectors(y_own, vr.at[0], vc.at[0], True)
    cps = multiply(1)
    dot = y_own * (out_r[0] + out_c[0] + ridge * y_own)
    for r in range(1, NR):
        dot += y_r[r] * out_r[r]
    for c in range(1, NC):
        dot += y_c[c] * out_c[c]
    total_send(1, [dot])
    sums = total_wait(0)
    for cp in ys.values():
        cp.wait_send()
    w_own = gathered(cps, 1) + ridge * y_own
    tt, ty, yy = sums[:, 0:1], sums[:, 1:2], sums[:, 2:3]
    alpha = tt / ty
    next_norm = alpha * alpha * yy - tt
    beta = next_norm / tt
    res1 = t_own - alpha * y_own
    dir2 = res1 + beta * t_own
    app2 = (1.0 + beta) * y_own - alpha * w_own
    part = (1.0 + beta) * ((1.0 + beta) * ty - 2.0 * alpha * yy)
    alpha2 = next_norm / (part + alpha * alpha * total_wait(1)[:, 0:1])
    coef_ref[...] = (alpha * t_own + alpha2 * dir2)[0:4, :]
    res_ref[...] = (res1 - alpha2 * app2)[0:4, :]


def body(points, targets, ridge_weight):
    vmem = pl.BlockSpec(memory_space=pltpu.VMEM)
    dma = pltpu.SemaphoreType.DMA
    out = jax.ShapeDtypeStruct((4, 128), f32)
    coef, res = pl.pallas_call(
        kernel,
        out_shape=(out, out),
        in_specs=[vmem, vmem, pl.BlockSpec(memory_space=pltpu.SMEM)],
        out_specs=(vmem, vmem),
        scratch_shapes=[
            pltpu.VMEM((NR, DIM, BLK), bf16), pltpu.VMEM((NC, DIM, BLK), bf16),
            pltpu.VMEM((NR, BLK, 256), bf16), pltpu.VMEM((NC, 256, BLK), bf16),
            pltpu.VMEM((NFULL + 16, BLK, BLK), bf16), pltpu.VMEM((256, 256), bf16),
            pltpu.VMEM((NR, 8, 128), f32), pltpu.VMEM((NC, 8, 128), f32),
            pltpu.VMEM((NR, 8, 128), f32), pltpu.VMEM((NC, 8, 128), f32),
            pltpu.VMEM((NR, 16, BLK), bf16), pltpu.VMEM((NC, 8, 128), f32),
            pltpu.VMEM((NR, BLK, 128), f32), pltpu.VMEM((NC, 16, BLK), f32),
            pltpu.VMEM((NR, 8, 128), f32), pltpu.VMEM((NC, 8, 128), f32),
            pltpu.VMEM((2, NR, 8, 128), f32), pltpu.VMEM((2, NC, 8, 128), f32),
            pltpu.VMEM((2, 1, 128), f32), pltpu.VMEM((2, 128, 1, 128), f32),
            dma((NR + NC,)), dma((NR,)), dma((NC,)),
            dma((NR + NC,)), dma((NR,)), dma((NC,)),
            dma((2, NR + NC)), dma((2, NR + NC)),
            dma((NR + NC,)), dma((NR,)), dma((NC,)),
            dma((2,)), dma((2,)), pltpu.SemaphoreType.REGULAR((3,)),
        ],
        compiler_params=pltpu.CompilerParams(
            collective_id=0, has_side_effects=True, vmem_limit_bytes=60 * 2 ** 20),
        name="cg",
    )(points.T, targets.reshape(4, 128), ridge_weight.reshape(1))
    return coef.reshape(-1), res.reshape(-1)


def solution(mesh):
    in_specs = (P("pts", None), P("pts"), P())
    out_specs = (P("pts"), P("pts"))
    return jax.shard_map(body, mesh=mesh, in_specs=in_specs, out_specs=out_specs, check_vma=False)
```
